32 devices in a mesh: ctx: 4 (over x, core), section: 8 (over z, y).
Axes of the slice: x: 2, y: 2, z: 4, core: 2. Of those that a mesh axis runs over, the one named last changes fastest.
Arguments:
- query_in: bfloat16 [8, 2, 512, 1024], P('section', None, 'ctx'), may hold values from -200 to 200
- key_in: bfloat16 [8, 2, 512, 128], P('section', None, 'ctx'), may hold values from -5 to 5
- value_in: bfloat16 [8, 2, 512, 128], P('section', None, 'ctx'), may hold values from -24 to 24
- forward_out: bfloat16 [8, 2, 512, 1024], P('section', None, 'ctx'), may hold values from -6 to 6
- log_sum: float32 [8, 2, 8, 512], P('section', None, None, 'ctx'), as said below
- grad_out: bfloat16 [8, 2, 512, 1024], P('section', None, 'ctx'), may hold values from -6 to 6
- block_order: int32 [8], replicated, may hold values from 0 to 7, each once
Outputs:
- grad_query: bfloat16 [8, 2, 512, 1024], P('section', None, 'ctx')
- grad_key: bfloat16 [8, 2, 512, 128], P('section', None, 'ctx')
- grad_value: bfloat16 [8, 2, 512, 128], P('section', None, 'ctx')
The draws below stay inside these ranges and needn't reach their ends.
Inputs may be any that keep to these rules, and one draw needn't show every extreme that they name: For every layer, micro-batch, head and row, log_sum is at least the logarithm of the sum of exp(score) over all key rows of that row's window, masked or not. block_order is a permutation: slot j, rows j * 64 to j * 64 + 63 of the token dimension, holds sequence positions block_order[j] * 64 onward in order.
All inputs are finite; a program needn't handle non-finite values.
Results may differ from the reference program's by a relative error of at most 0.008.
Values may be sent and summed in bfloat16 or wider, within the bound.
A program may use at most 64 MiB of HBM per device.

```python
import jax
import jax.numpy as jnp
from jax import lax

HEADS = 8
HEAD = 128
TOK_DEV = 128
MICRO = 2
WINDOW = 3
SECTIONS = 8
TOKENS = 512
HALF = 64
BLOCKS = 8


def pair_item(key, index):
    item_key = jax.random.fold_in(key, index)
    keys_raw = jnp.clip(jax.random.normal(jax.random.fold_in(item_key, 11), (TOKENS, HEAD), jnp.float32), -5.0, 5.0)
    queries = jnp.clip(jax.random.normal(jax.random.fold_in(item_key, 12), (TOKENS, HEADS, HEAD), jnp.float32), -5.0, 5.0)
    return (queries.reshape(TOKENS, HEADS * HEAD), keys_raw, item_key)


def item_list():
    return jnp.arange(SECTIONS * MICRO, dtype=jnp.int32)


def draw_query_in(key, part):
    items = lax.map(lambda index: pair_item(key, index)[0].astype(jnp.bfloat16), item_list())
    return items.reshape(SECTIONS, MICRO, TOKENS, HEADS * HEAD)


def draw_key_in(key, part):
    items = lax.map(lambda index: pair_item(key, index)[1].astype(jnp.bfloat16), item_list())
    return items.reshape(SECTIONS, MICRO, TOKENS, HEAD)


def log_item(key, index):
    queries, keys_raw, item_key = pair_item(key, index)
    shards = TOKENS // TOK_DEV
    query_low = queries.astype(jnp.bfloat16).astype(jnp.float32).reshape(shards, TOK_DEV, HEADS, HEAD)
    key_low = keys_raw.astype(jnp.bfloat16).astype(jnp.float32).reshape(shards, TOK_DEV, HEAD)
    window_keys = jnp.concatenate([jnp.roll(key_low, offset, axis=0) for offset in range(WINDOW)], axis=1)
    scores = jnp.einsum('cqhd,ckd->chqk', query_low, window_keys, precision=lax.Precision.HIGHEST) / jnp.sqrt(jnp.float32(HEAD))
    top = jnp.max(scores, axis=-1)
    total = jnp.sum(jnp.exp(scores - top[..., None]), axis=-1)
    extra = jnp.exp(jax.random.uniform(jax.random.fold_in(item_key, 14), (shards, HEADS, TOK_DEV), jnp.float32, jnp.log(0.1), jnp.log(2.0)))
    log_rows = top + jnp.log(total + extra)
    return jnp.transpose(log_rows, (1, 0, 2)).reshape(HEADS, TOKENS)


def draw_log_sum(key, part):
    items = lax.map(lambda index: log_item(key, index), item_list())
    return items.reshape(SECTIONS, MICRO, HEADS, TOKENS)


def shard_levels(key, dims, cuts, low, largest):
    def one(axis_at, parts):
        heights = jax.random.uniform(jax.random.fold_in(jax.random.fold_in(key, 6), axis_at), (parts,), jnp.float32, low / len(cuts), largest / len(cuts))
        return jnp.repeat(jnp.exp(heights), dims[axis_at] // parts).reshape((-1,) + (1,) * (len(dims) - axis_at - 1))

    factor_of = one(*cuts[0])
    for cut in cuts[1:]:
        factor_of = factor_of * one(*cut)
    return factor_of


def gaussian(key, shape, deviation, reach, split=(), kind=jnp.bfloat16):
    drawn = deviation * jax.random.normal(key, shape, jnp.float32)
    if split:
        drawn = drawn * shard_levels(key, shape, split, -0.22, 0.18)
    return jnp.clip(drawn, -reach, reach).astype(kind)


def setup_inputs(seed: int = 0) -> dict:
    key_of = jax.random.split(jax.random.key(seed), 8)
    query_in = draw_query_in(jax.random.fold_in(key_of[7], 71), 0)
    key_in = draw_key_in(jax.random.fold_in(key_of[7], 71), 0)
    value_in = gaussian(key_of[2], (SECTIONS, MICRO, TOKENS, HEAD), 4.0, 24.0, ((0, 8), (2, 4)))
    forward_out = gaussian(key_of[3], (SECTIONS, MICRO, TOKENS, HEADS * HEAD), 1.0, 6.0, ((0, 8), (2, 4)))
    log_sum = draw_log_sum(jax.random.fold_in(key_of[7], 71), 0)
    grad_out = gaussian(key_of[5], (SECTIONS, MICRO, TOKENS, HEADS * HEAD), 1.0, 6.0, ((0, 8), (2, 4)))
    block_order = jax.random.permutation(key_of[6], BLOCKS).astype(jnp.int32)
    return {"query_in": query_in, "key_in": key_in, "value_in": value_in, "forward_out": forward_out, "log_sum": log_sum, "grad_out": grad_out, "block_order": block_order}


def place_rows(block_order, length, half_rows):
    row_ids = jnp.arange(length, dtype=jnp.int32)
    slot_ids = row_ids // half_rows
    lookup = (slot_ids[:, None] == jnp.arange(block_order.shape[0], dtype=jnp.int32)[None, :]).astype(jnp.int32)
    return lax.optimization_barrier(jnp.sum(lookup * block_order[None, :], axis=1)) * half_rows + row_ids % half_rows

def round_keep(values_in):
    return lax.optimization_barrier(values_in.astype(jnp.bfloat16)).astype(jnp.float32)

def layer_backward(query_rows, key_rows, value_rows, saved_out, saved_log, upstream, places):
    shards = TOKENS // TOK_DEV
    factor = 1.0 / jnp.sqrt(jnp.float32(HEAD))
    query_heads = query_rows.reshape(shards, TOK_DEV, HEADS, HEAD).astype(jnp.float32)
    grad_heads = upstream.reshape(shards, TOK_DEV, HEADS, HEAD).astype(jnp.float32)
    out_heads = saved_out.reshape(shards, TOK_DEV, HEADS, HEAD).astype(jnp.float32)
    row_dot = jnp.transpose(lax.optimization_barrier(jnp.sum(grad_heads * out_heads, axis=-1)), (0, 2, 1))
    log_rows = jnp.transpose(saved_log.reshape(HEADS, shards, TOK_DEV), (1, 0, 2))
    key_float = key_rows.reshape(shards, TOK_DEV, HEAD).astype(jnp.float32)
    value_float = value_rows.reshape(shards, TOK_DEV, HEAD).astype(jnp.float32)
    place_shards = places.reshape(shards, TOK_DEV)
    grad_query = jnp.zeros((shards, TOK_DEV, HEADS, HEAD), jnp.float32)
    grad_key = jnp.zeros((shards, TOK_DEV, HEAD), jnp.float32)
    grad_value = jnp.zeros((shards, TOK_DEV, HEAD), jnp.float32)
    for offset in range(WINDOW):
        key_near = jnp.roll(key_float, offset, axis=0)
        value_near = jnp.roll(value_float, offset, axis=0)
        place_near = jnp.roll(place_shards, offset, axis=0)
        scores = jnp.einsum('cqhd,ckd->chqk', query_heads, key_near) * factor
        visible = place_shards[:, :, None] >= place_near[:, None, :]
        probs = jnp.where(visible[:, None], jnp.exp(scores - log_rows[..., None]), 0.0)
        grad_probs = jnp.einsum('cqhd,ckd->chqk', grad_heads, value_near)
        grad_scores = round_keep(probs * (grad_probs - row_dot[..., None]))
        probs_low = round_keep(probs)
        grad_query = grad_query + jnp.einsum('chqk,ckd->cqhd', grad_scores, key_near) * factor
        key_terms = jnp.einsum('chqk,cqhd->ckd', grad_scores, query_heads) * factor
        value_terms = jnp.einsum('chqk,cqhd->ckd', probs_low, grad_heads)
        grad_key = grad_key + jnp.roll(key_terms, -offset, axis=0)
        grad_value = grad_value + jnp.roll(value_terms, -offset, axis=0)
    return (grad_query.reshape(TOKENS, HEADS * HEAD).astype(jnp.bfloat16), grad_key.reshape(TOKENS, HEAD).astype(jnp.bfloat16), grad_value.reshape(TOKENS, HEAD).astype(jnp.bfloat16))

def reference(query_in, key_in, value_in, forward_out, log_sum, grad_out, block_order):
    places = place_rows(block_order, TOKENS, HALF)

    def run_layer(items):
        return layer_backward(items[0], items[1], items[2], items[3], items[4], items[5], places)
    first = lax.map(run_layer, (query_in[:, 0], key_in[:, 0], value_in[:, 0], forward_out[:, 0], log_sum[:, 0], grad_out[:, 0]))
    passed = jnp.concatenate([first[0][1:], jnp.zeros_like(first[0][:1])], axis=0)
    upstream = (grad_out[:, 1].astype(jnp.float32) + passed.astype(jnp.float32)).astype(jnp.bfloat16)
    second = lax.map(run_layer, (query_in[:, 1], key_in[:, 1], value_in[:, 1], forward_out[:, 1], log_sum[:, 1], upstream))
    grad_query = jnp.stack([first[0], second[0]], axis=1)
    grad_key = jnp.stack([first[1], second[1]], axis=1)
    grad_value = jnp.stack([first[2], second[2]], axis=1)
    return (grad_query, grad_key, grad_value)
```

```python
import functools
import math

import jax
import jax.numpy as jnp
from jax import lax
from jax.experimental import pallas as pl
from jax.experimental.pallas import tpu as pltpu
from jax.sharding import PartitionSpec as P

WINDOW = 3
LOG2E = math.log2(math.e)
HIDE = -1e30


def dot(a, b, dims):
    return lax.dot_general(a, b, (dims, ((), ())), preferred_element_type=jnp.float32)


def kernel(
    members, sections, blocks,
    order_hbm, q_hbm, k_hbm, v_hbm, fo_hbm, go_hbm, log_hbm,
    dq, kv_out,
    rows_in, logs, kv, bias, passed, own, part, back, dq_own, ds, pr, pf, order,
    order_sem, rows_sem, log_sem, kv_sem,
    kv_send, kv_recv, part_send, part_recv, hop_send, hop_recv,
):
    _, micro, rows, width = rows_in.shape
    q, go, fo = rows_in.at[0], rows_in.at[1], rows_in.at[2]
    head = kv.shape[-1]
    chunks, _, wide = passed.shape
    group = wide // head
    span = group * rows
    factor = 1.0 / math.sqrt(head)
    me = lax.axis_index("ctx")
    sec = lax.axis_index("section")
    peer = lambda offset: {"ctx": lax.rem(me + offset + members, members)}
    below = {"section": jnp.maximum(sec - 1, 0)}
    above = {"section": jnp.minimum(sec + 1, sections - 1)}
    has_below = sec > 0
    has_above = sec < sections - 1

    barrier = pltpu.get_barrier_semaphore()
    near = sorted({o % members for o in range(1 - WINDOW, WINDOW)} - {0})
    for o in near:
        pl.semaphore_signal(barrier, inc=1, device_id=peer(o), device_id_type=pl.DeviceIdType.MESH)

    @pl.when(has_above)
    def _():
        pl.semaphore_signal(barrier, inc=1, device_id=above, device_id_type=pl.DeviceIdType.MESH)

    def arrived(ref, sem):
        pltpu.make_async_copy(ref, ref, sem).wait()

    for m in range(micro):
        for which, source in enumerate((k_hbm, v_hbm)):
            pltpu.make_async_copy(source.at[0, m], kv.at[m, 0, which], kv_sem.at[m]).start()
    order_load = pltpu.make_async_copy(order_hbm, order, order_sem)
    order_load.start()
    log_load = pltpu.make_async_copy(log_hbm.at[0], logs, log_sem)
    log_load.start()
    for which, source in enumerate((q_hbm, go_hbm, fo_hbm)):
        pltpu.make_async_copy(source.at[0], rows_in.at[which], rows_sem).start()

    half = members * rows // blocks
    per = rows // half
    lane = lax.broadcasted_iota(jnp.int32, (half, rows), 1)
    down = lax.broadcasted_iota(jnp.int32, (half, rows), 0)
    q_place = lax.rem(lane, half)
    order_load.wait()
    for b in range(per):
        base = order[me * per + b] * half
        q_place = q_place + jnp.where(lane // half == b, base, 0)
    for o in range(WINDOW):
        source = lax.rem(me - o + members, members)
        for b in range(per):
            k_place = down + order[source * per + b] * half
            tile = jnp.where(k_place <= q_place, 0.0, HIDE)
            for g in range(group):
                bias[pl.ds(o * rows + b * half, half), pl.ds(g * rows, rows)] = tile

    @pl.when(jnp.logical_not(has_above))
    def _():
        passed[...] = jnp.zeros_like(passed)

    if True:
        pl.semaphore_wait(barrier, len(near) + has_below.astype(jnp.int32))

    others = pl.ds(1, WINDOW - 1)

    def send_kv(m):
        for o in range(WINDOW - 1, 0, -1):
            pltpu.make_async_remote_copy(
                src_ref=kv.at[m, 0], dst_ref=kv.at[m, o],
                send_sem=kv_send, recv_sem=kv_recv.at[m],
                device_id=peer(o), device_id_type=pl.DeviceIdType.MESH,
            ).start()

    arrived(kv.at[0, 0], kv_sem.at[0])
    send_kv(0)

    ones = jnp.ones((8, head), jnp.bfloat16)
    near_rows = pl.ds(rows, (WINDOW - 1) * rows)
    own_rows = pl.ds(0, rows)

    def split(block):
        return jnp.concatenate([block[:, g * head:(g + 1) * head] for g in range(group)], axis=0)

    def stack(block):
        return jnp.concatenate([block[:, h * head:(h + 1) * head] for h in range(width // head)], axis=0)

    def cols(c):
        return pl.ds(c * wide, wide)

    def lanes(c):
        return pl.ds(c * span, span)

    def queries(m, c):
        return split(q[m, :, cols(c)])

    def row_dots(m, c, upstream):
        product = upstream.astype(jnp.float32) * split(fo[m, :, cols(c)]).astype(jnp.float32)
        high = product.astype(jnp.bfloat16)
        low = (product - high.astype(jnp.float32)).astype(jnp.bfloat16)
        return (dot(ones, high, ((1,), (1,))) + dot(ones, low, ((1,), (1,))))[0:1]

    def probs_of(m, c, keys, where):
        log_row = jnp.concatenate(
            [logs[m, pl.ds(c * group + g, 1), :] for g in range(group)], axis=1
        ) * LOG2E
        scores = dot(keys, queries(m, c), ((1,), (1,)))
        return jnp.exp2(scores * (factor * LOG2E) - log_row + bias[where])

    def far(m, which):
        return jnp.concatenate([kv[m, o, which] for o in range(1, WINDOW)], axis=0)

    def grads_of(probs, values, upstream, row_dot):
        return (probs * (dot(values, upstream, ((1,), (1,))) - row_dot)).astype(jnp.bfloat16)

    def put_dq(m, c, grad_query):
        for g in range(group):
            dq[m, c, :, pl.ds(g * head, head)] = grad_query[g * rows:(g + 1) * rows].astype(jnp.bfloat16)

    def hop(c):
        return pltpu.make_async_remote_copy(
            src_ref=dq.at[0, c], dst_ref=passed.at[c],
            send_sem=hop_send, recv_sem=hop_recv.at[c],
            device_id=below, device_id_type=pl.DeviceIdType.MESH,
        )

    def send_parts(m, dk, dv):
        for o in range(WINDOW - 1, 0, -1):
            for which, total in enumerate((dk, dv)):
                part[m, o - 1, which] = total[(o - 1) * rows:o * rows].astype(jnp.bfloat16)
            pltpu.make_async_remote_copy(
                src_ref=part.at[m, o - 1], dst_ref=back.at[m, o - 1],
                send_sem=part_send, recv_sem=part_recv.at[m],
                device_id=peer(-o), device_id_type=pl.DeviceIdType.MESH,
            ).start()

    def finish(m):
        arrived(back.at[m], part_recv.at[m])
        for which in range(2):
            total = own[m, which]
            for o in range(1, WINDOW):
                total = total + back[m, o - 1, which].astype(jnp.float32)
            kv_out[m, which] = total.astype(jnp.bfloat16)

    if True:
        log_load.wait()
        arrived(rows_in, rows_sem)
    keys, values = kv[0, 0, 0], kv[0, 0, 1]
    row_dot = []
    if True:
        for c in range(chunks):
            upstream = split(go[0, :, cols(c)])
            row_dot.append(row_dots(0, c, upstream))
            probs = probs_of(0, c, keys, own_rows)
            grads = grads_of(probs, values, upstream, row_dot[c])
            pr[own_rows, lanes(c)] = probs.astype(jnp.bfloat16)
            ds[own_rows, lanes(c)] = grads
            dq_own[c] = dot(grads, keys, ((0,), (0,)))

    if True:
        arrived(kv.at[0, others], kv_recv.at[0])
    for m in range(1, micro):
        arrived(kv.at[m, 0], kv_sem.at[m])
        send_kv(m)

    keys, values = far(0, 0), far(0, 1)
    for c in range(chunks):
        if True:
            upstream = split(go[0, :, cols(c)])
            probs = probs_of(0, c, keys, near_rows)
            grads = grads_of(probs, values, upstream, row_dot[c])
            pr[near_rows, lanes(c)] = probs.astype(jnp.bfloat16)
            ds[near_rows, lanes(c)] = grads
            put_dq(0, c, (dq_own[c] + dot(grads, keys, ((0,), (0,)))) * factor)

            @pl.when(has_below)
            def _(c=c):
                hop(c).start()

    if True:
        all_queries, all_upstream = stack(q[0]), stack(go[0])
        dk = dot(ds[...], all_queries, ((1,), (0,))) * factor
        dv = dot(pr[...], all_upstream, ((1,), (0,)))
        send_parts(0, dk[rows:], dv[rows:])
        own[0, 0] = dk[:rows]
        own[0, 1] = dv[:rows]

    for m in range(1, micro):
        if True:
            arrived(kv.at[m, others], kv_recv.at[m])
        keys = jnp.concatenate([kv[m, o, 0] for o in range(WINDOW)], axis=0)
        if True:
            for c in range(chunks):
                pf[:, lanes(c)] = probs_of(m, c, keys, pl.ds(0, WINDOW * rows))

        far_values, own_values = far(m, 1), kv[m, 0, 1]
        dk_far = dv_far = dk_own = dv_own = None
        for c in range(chunks):
            if m == 1:
                @pl.when(has_above)
                def _(c=c):
                    if True:
                        hop(c).wait_recv()
            if True:
                chunk = queries(m, c)
                upstream = split((
                    go[m, :, cols(c)].astype(jnp.float32) + passed[c].astype(jnp.float32)
                ).astype(jnp.bfloat16))
                dots = row_dots(m, c, upstream)
                probs = pf[near_rows, lanes(c)]
                grads = grads_of(probs, far_values, upstream, dots)
                dk = dot(grads, chunk, ((1,), (0,)))
                dv = dot(probs.astype(jnp.bfloat16), upstream, ((1,), (0,)))
                dk_far = dk if dk_far is None else dk_far + dk
                dv_far = dv if dv_far is None else dv_far + dv
                if c == chunks - 1:
                    send_parts(m, dk_far * factor, dv_far)
            if True:
                probs = pf[own_rows, lanes(c)]
                own_grads = grads_of(probs, own_values, upstream, dots)
                dk = dot(own_grads, chunk, ((1,), (0,)))
                dv = dot(probs.astype(jnp.bfloat16), upstream, ((1,), (0,)))
                dk_own = dk if dk_own is None else dk_own + dk
                dv_own = dv if dv_own is None else dv_own + dv
                put_dq(m, c, dot(jnp.concatenate([own_grads, grads], axis=0), keys, ((0,), (0,))) * factor)
        own[m, 0] = dk_own * factor
        own[m, 1] = dv_own

    for m in range(micro):
        if True:
            finish(m)
    arrived(kv.at[:, others], kv_send)
    arrived(part, part_send)

    @pl.when(has_below)
    def _():
        arrived(passed, hop_send)


def writer(dq, kv_out, dq_hbm, dk_hbm, dv_hbm, sem):
    micro, chunks, _, wide = dq.shape
    for m in range(micro):
        for c in range(chunks):
            pltpu.make_async_copy(
                dq.at[m, c], dq_hbm.at[0, m, :, pl.ds(c * wide, wide)], sem.at[0]
            ).start()
        for which, target in enumerate((dk_hbm, dv_hbm)):
            pltpu.make_async_copy(kv_out.at[m, which], target.at[0, m], sem.at[1]).start()
    pltpu.make_async_copy(dq, dq, sem.at[0]).wait()
    pltpu.make_async_copy(kv_out, kv_out, sem.at[1]).wait()


def solution(mesh):
    members = mesh.shape["ctx"]
    sections = mesh.shape["section"]
    in_specs = (
        P("section", None, "ctx", None),
        P("section", None, "ctx", None),
        P("section", None, "ctx", None),
        P("section", None, "ctx", None),
        P("section", None, None, "ctx"),
        P("section", None, "ctx", None),
        P(),
    )
    out_specs = (
        P("section", None, "ctx", None),
        P("section", None, "ctx", None),
        P("section", None, "ctx", None),
    )

    def shards(query_in, key_in, value_in, forward_out, log_sum, grad_out, block_order):
        _, micro, rows, width = query_in.shape
        head = key_in.shape[3]
        heads = width // head
        group = 2 if heads % 2 == 0 else 1
        chunks = heads // group
        wide = group * head
        low, full = jnp.bfloat16, jnp.float32
        dma = pltpu.SemaphoreType.DMA
        others = WINDOW - 1
        dq, kv_out = pl.pallas_call(
            functools.partial(kernel, members, sections, block_order.shape[0]),
            out_shape=(
                pltpu.VMEM((micro, chunks, rows, wide), low),
                pltpu.VMEM((micro, 2, rows, head), low),
            ),
            in_specs=[pl.BlockSpec(memory_space=pl.ANY)] * 7,
            out_specs=[pl.BlockSpec(memory_space=pltpu.VMEM)] * 2,
            scratch_shapes=[
                pltpu.VMEM((3, micro, rows, width), low),
                pltpu.VMEM((micro, heads, rows), full),
                pltpu.VMEM((micro, WINDOW, 2, rows, head), low),
                pltpu.VMEM((WINDOW * rows, group * rows), full),
                pltpu.VMEM((chunks, rows, wide), low),
                pltpu.VMEM((micro, 2, rows, head), full),
                pltpu.VMEM((micro, others, 2, rows, head), low),
                pltpu.VMEM((micro, others, 2, rows, head), low),
                pltpu.VMEM((chunks, group * rows, head), full),
                pltpu.VMEM((WINDOW * rows, heads * rows), low),
                pltpu.VMEM((WINDOW * rows, heads * rows), low),
                pltpu.VMEM((WINDOW * rows, heads * rows), full),
                pltpu.SMEM(block_order.shape, jnp.int32),
                dma, dma, dma, dma((micro,)),
                dma, dma((micro,)), dma, dma((micro,)), dma, dma((chunks,)),
            ],
            compiler_params=pltpu.CompilerParams(collective_id=0, has_side_effects=True),
        )(block_order, query_in, key_in, value_in, forward_out, grad_out, log_sum)
        return pl.pallas_call(
            writer,
            out_shape=(
                jax.ShapeDtypeStruct(query_in.shape, low),
                jax.ShapeDtypeStruct(key_in.shape, low),
                jax.ShapeDtypeStruct(value_in.shape, low),
            ),
            in_specs=[pl.BlockSpec(memory_space=pltpu.VMEM)] * 2,
            out_specs=[pl.BlockSpec(memory_space=pl.ANY)] * 3,
            scratch_shapes=[dma((2,))],
        )(*(pltpu.with_memory_space_constraint(x, pltpu.VMEM) for x in (dq, kv_out)))

    return jax.shard_map(shards, mesh=mesh, in_specs=in_specs, out_specs=out_specs, check_vma=False)
```

```python
import functools
import math

import jax
import jax.numpy as jnp
from jax import lax
from jax.experimental import pallas as pl
from jax.experimental.pallas import tpu as pltpu
from jax.sharding import PartitionSpec as P

WINDOW = 3
KEEP = 2
AFTER = {2: 1, 3: 1}
LOG2E = math.log2(math.e)
HIDE = -1e30


def dot(a, b, dims):
    return lax.dot_general(a, b, (dims, ((), ())), preferred_element_type=jnp.float32)


def kernel(
    members, sections, blocks,
    order_hbm, q_hbm, k_hbm, v_hbm, fo_hbm, go_hbm, log_hbm,
    dq, kv_out,
    rows_in, logs, kv, bias, passed, own, part, back, dq_own, ds, pr, pf, far_sum, order,
    order_sem, rows_sem, log_sem, kv_sem,
    kv_send, k_recv, v_recv, part_send, part_recv, relay_recv, hop_send, hop_recv,
):
    _, micro, rows, width = rows_in.shape
    q, go, fo = rows_in.at[0], rows_in.at[1], rows_in.at[2]
    head = kv.shape[-1]
    chunks, _, wide = passed.shape
    group = wide // head
    span = group * rows
    factor = 1.0 / math.sqrt(head)
    me = lax.axis_index("ctx")
    sec = lax.axis_index("section")
    peer = lambda offset: {"ctx": lax.rem(me + offset + members, members)}
    below = {"section": jnp.maximum(sec - 1, 0)}
    above = {"section": jnp.minimum(sec + 1, sections - 1)}
    has_below = sec > 0
    has_above = sec < sections - 1
    first = lax.rem(me, 2) == 0

    barrier = pltpu.get_barrier_semaphore()
    near = sorted({o % members for o in range(1 - WINDOW, WINDOW)} - {0})
    for o in near:
        pl.semaphore_signal(barrier, inc=1, device_id=peer(o), device_id_type=pl.DeviceIdType.MESH)

    @pl.when(has_above)
    def _():
        pl.semaphore_signal(barrier, inc=1, device_id=above, device_id_type=pl.DeviceIdType.MESH)

    def arrived(ref, sem):
        pltpu.make_async_copy(ref, ref, sem).wait()

    for m in range(micro):
        for which, source in enumerate((k_hbm, v_hbm)):
            pltpu.make_async_copy(source.at[0, m], kv.at[m, 0, which], kv_sem.at[m]).start()
    order_load = pltpu.make_async_copy(order_hbm, order, order_sem)
    order_load.start()
    log_load = pltpu.make_async_copy(log_hbm.at[0], logs, log_sem)
    log_load.start()
    for which, source in enumerate((q_hbm, go_hbm, fo_hbm)):
        pltpu.make_async_copy(source.at[0], rows_in.at[which], rows_sem).start()

    if True:
        pl.semaphore_wait(barrier, len(near) + has_below.astype(jnp.int32))

    others = pl.ds(1, WINDOW - 1)
    far_recv = (k_recv, v_recv)

    def move_kv(m, source, which, offset, slot):
        pltpu.make_async_remote_copy(
            src_ref=kv.at[m, source, which], dst_ref=kv.at[m, slot, which],
            send_sem=kv_send, recv_sem=far_recv[which].at[m],
            device_id=peer(offset), device_id_type=pl.DeviceIdType.MESH,
        ).start()

    def send_kv(m):
        for which in range(2):
            move_kv(m, 0, which, 2, 2)

        @pl.when(first)
        def _():
            for which in range(2):
                move_kv(m, 0, which, 1, 1)

    def take_kv(m, which):
        arrived(kv.at[m, others, which], far_recv[which].at[m])

        @pl.when(jnp.logical_not(first))
        def _():
            move_kv(m, 2, which, -1, 1)

    arrived(kv.at[0, 0], kv_sem.at[0])
    send_kv(0)

    half = members * rows // blocks
    per = rows // half
    lane = lax.broadcasted_iota(jnp.int32, (half, rows), 1)
    down = lax.broadcasted_iota(jnp.int32, (half, rows), 0)
    q_place = lax.rem(lane, half)
    order_load.wait()
    for b in range(per):
        base = order[me * per + b] * half
        q_place = q_place + jnp.where(lane // half == b, base, 0)
    for o in range(WINDOW):
        source = lax.rem(me - o + members, members)
        for b in range(per):
            k_place = down + order[source * per + b] * half
            tile = jnp.where(k_place <= q_place, 0.0, HIDE)
            for g in range(group):
                bias[pl.ds(o * rows + b * half, half), pl.ds(g * rows, rows)] = tile

    @pl.when(jnp.logical_not(has_above))
    def _():
        passed[...] = jnp.zeros_like(passed)

    ones = jnp.ones((8, head), jnp.bfloat16)
    near_rows = pl.ds(rows, (WINDOW - 1) * rows)
    own_rows = pl.ds(0, rows)

    def split(block):
        return jnp.concatenate([block[:, g * head:(g + 1) * head] for g in range(group)], axis=0)

    def stack(block):
        return jnp.concatenate([block[:, h * head:(h + 1) * head] for h in range(width // head)], axis=0)

    def cols(c):
        return pl.ds(c * wide, wide)

    def lanes(c):
        return pl.ds(c * span, span)

    def queries(m, c):
        return split(q[m, :, cols(c)])

    def row_dots(m, c, upstream):
        product = upstream.astype(jnp.float32) * split(fo[m, :, cols(c)]).astype(jnp.float32)
        high = product.astype(jnp.bfloat16)
        low = (product - high.astype(jnp.float32)).astype(jnp.bfloat16)
        return (dot(ones, high, ((1,), (1,))) + dot(ones, low, ((1,), (1,))))[0:1]

    def probs_of(m, c, keys, where):
        log_row = jnp.concatenate(
            [logs[m, pl.ds(c * group + g, 1), :] for g in range(group)], axis=1
        ) * LOG2E
        scores = dot(keys, queries(m, c), ((1,), (1,)))
        return jnp.exp2(scores * (factor * LOG2E) - log_row + bias[where])

    def far(m, which):
        return jnp.concatenate([kv[m, o, which] for o in range(1, WINDOW)], axis=0)

    def grads_of(probs, values, upstream, row_dot):
        return (probs * (dot(values, upstream, ((1,), (1,))) - row_dot)).astype(jnp.bfloat16)

    def put_dq(m, c, grad_query):
        for g in range(group):
            dq[m, c, :, pl.ds(g * head, head)] = grad_query[g * rows:(g + 1) * rows].astype(jnp.bfloat16)

    def hop(c):
        return pltpu.make_async_remote_copy(
            src_ref=dq.at[0, c], dst_ref=passed.at[c],
            send_sem=hop_send, recv_sem=hop_recv.at[c],
            device_id=below, device_id_type=pl.DeviceIdType.MESH,
        )

    def send_part(m, o, offset, recv_sem):
        pltpu.make_async_remote_copy(
            src_ref=part.at[m, o - 1], dst_ref=back.at[m, o - 1],
            send_sem=part_send, recv_sem=recv_sem,
            device_id=peer(offset), device_id_type=pl.DeviceIdType.MESH,
        ).start()

    def send_parts(m, dk, dv):
        for o in range(WINDOW - 1, 0, -1):
            for which, total in enumerate((dk, dv)):
                part[m, o - 1, which] = total[(o - 1) * rows:o * rows].astype(jnp.bfloat16)
            send_part(m, o, -o, part_recv.at[m])

    def finish(m):
        if m < micro - 1:
            arrived(back.at[m], part_recv.at[m])
        else:
            @pl.when(first)
            def _():
                arrived(back.at[m], part_recv.at[m])

            @pl.when(jnp.logical_not(first))
            def _():
                arrived(back.at[m, 1], part_recv.at[m])
        for which in range(2):
            total = own[m, which] + back[m, 1, which].astype(jnp.float32)
            beside = back[m, 0, which].astype(jnp.float32)
            if m == micro - 1:
                beside = jnp.where(first, beside, 0.0)
            kv_out[m, which] = (total + beside).astype(jnp.bfloat16)

    if True:
        log_load.wait()
        arrived(rows_in, rows_sem)
    keys, values = kv[0, 0, 0], kv[0, 0, 1]
    row_dot = []
    if True:
        for c in range(chunks):
            upstream = split(go[0, :, cols(c)])
            row_dot.append(row_dots(0, c, upstream))
            probs = probs_of(0, c, keys, own_rows)
            grads = grads_of(probs, values, upstream, row_dot[c])
            pr[own_rows, lanes(c)] = probs.astype(jnp.bfloat16)
            ds[own_rows, lanes(c)] = grads
            dq_own[c] = dot(grads, keys, ((0,), (0,)))

    if True:
        take_kv(0, 0)
    keys = far(0, 0)
    if True:
        for c in range(chunks):
            pf[near_rows, lanes(c)] = probs_of(0, c, keys, near_rows)
    if True:
        take_kv(0, 1)
    for m in range(1, micro):
        arrived(kv.at[m, 0], kv_sem.at[m])
        send_kv(m)
    values = far(0, 1)
    for c in range(chunks):
        if True:
            upstream = split(go[0, :, cols(c)])
            probs = pf[near_rows, lanes(c)]
            grads = grads_of(probs, values, upstream, row_dot[c])
            ds[near_rows, lanes(c)] = grads
            put_dq(0, c, (dq_own[c] + dot(grads, keys, ((0,), (0,)))) * factor)

            @pl.when(has_below if c < KEEP else jnp.logical_and(has_below, first))
            def _(c=c):
                hop(c).start()

            pr[near_rows, lanes(c)] = probs.astype(jnp.bfloat16)

    if True:
        all_queries, all_upstream = stack(q[0]), stack(go[0])
        dk = dot(ds[...], all_queries, ((1,), (0,))) * factor
        dv = dot(pr[...], all_upstream, ((1,), (0,)))
        send_parts(0, dk[rows:], dv[rows:])
        own[0, 0] = dk[:rows]
        own[0, 1] = dv[:rows]

    for m in range(1, micro):
        if True:
            for which in range(2):
                take_kv(m, which)
        keys = jnp.concatenate([kv[m, o, 0] for o in range(WINDOW)], axis=0)
        if True:
            for c in range(chunks):
                pf[:, lanes(c)] = probs_of(m, c, keys, pl.ds(0, WINDOW * rows))

        far_values, own_values = far(m, 1), kv[m, 0, 1]
        all_queries = stack(q[m])
        ready = (chunks - 1) * span
        dots, ups = [], []
        for c in range(chunks):
            if c == chunks - 1:
                if True:
                    early = pl.ds(0, ready)
                    far_sum[0] = dot(ds[near_rows, early], all_queries[:ready], ((1,), (0,)))
                    far_sum[1] = dot(pr[near_rows, early], jnp.concatenate(ups, axis=0), ((1,), (0,)))
            if m == 1:
                @pl.when(has_above)
                def _(c=c):
                    if True:
                        hop(c).wait_recv()
            if True:
                upstream = split((
                    go[m, :, cols(c)].astype(jnp.float32) + passed[c].astype(jnp.float32)
                ).astype(jnp.bfloat16))
                ups.append(upstream)
                dots.append(row_dots(m, c, upstream))
                probs = pf[near_rows, lanes(c)]
                grads = grads_of(probs, far_values, upstream, dots[c])
                ds[near_rows, lanes(c)] = grads
                probs = probs.astype(jnp.bfloat16)
                if c < chunks - 1:
                    pr[near_rows, lanes(c)] = probs
                else:
                    dv = far_sum[1] + dot(probs, upstream, ((1,), (0,)))
                    dk = (far_sum[0] + dot(grads, all_queries[ready:], ((1,), (0,)))) * factor
                    for which, total in enumerate((dk, dv)):
                        part[m, 0, which] = total[:rows].astype(jnp.bfloat16)

                    @pl.when(first)
                    def _():
                        send_part(m, 1, 1, relay_recv)
                        for which, total in enumerate((dk, dv)):
                            part[m, 1, which] = total[rows:].astype(jnp.bfloat16)
                        send_part(m, 2, -2, part_recv.at[m])

                    @pl.when(jnp.logical_not(first))
                    def _():
                        send_part(m, 1, -1, part_recv.at[m])
                        arrived(back.at[m, 0], relay_recv)
                        for which, total in enumerate((dk, dv)):
                            both = total[rows:] + back[m, 0, which].astype(jnp.float32)
                            part[m, 1, which] = both.astype(jnp.bfloat16)
                        send_part(m, 2, -2, part_recv.at[m])
            for later, after in AFTER.items():
                if after == c:
                    @pl.when(jnp.logical_and(has_below, jnp.logical_not(first)))
                    def _(later=later):
                        hop(later).start()
        if True:
            for c in range(chunks):
                probs = pf[own_rows, lanes(c)]
                ds[own_rows, lanes(c)] = grads_of(probs, own_values, ups[c], dots[c])
                pr[own_rows, lanes(c)] = probs.astype(jnp.bfloat16)
                put_dq(m, c, dot(ds[:, lanes(c)], keys, ((0,), (0,))) * factor)
            own[m, 0] = dot(ds[own_rows, :], all_queries, ((1,), (0,))) * factor
            own[m, 1] = dot(pr[own_rows, :], jnp.concatenate(ups, axis=0), ((1,), (0,)))

    for m in range(micro):
        if True:
            finish(m)
    arrived(kv.at[:, others], kv_send)
    arrived(part, part_send)

    @pl.when(has_below)
    def _():
        arrived(passed, hop_send)


def writer(dq, kv_out, dq_hbm, dk_hbm, dv_hbm, sem):
    micro, chunks, _, wide = dq.shape
    for m in range(micro):
        for c in range(chunks):
            pltpu.make_async_copy(
                dq.at[m, c], dq_hbm.at[0, m, :, pl.ds(c * wide, wide)], sem.at[0]
            ).start()
        for which, target in enumerate((dk_hbm, dv_hbm)):
            pltpu.make_async_copy(kv_out.at[m, which], target.at[0, m], sem.at[1]).start()
    pltpu.make_async_copy(dq, dq, sem.at[0]).wait()
    pltpu.make_async_copy(kv_out, kv_out, sem.at[1]).wait()


def solution(mesh):
    members = mesh.shape["ctx"]
    sections = mesh.shape["section"]
    in_specs = (
        P("section", None, "ctx", None),
        P("section", None, "ctx", None),
        P("section", None, "ctx", None),
        P("section", None, "ctx", None),
        P("section", None, None, "ctx"),
        P("section", None, "ctx", None),
        P(),
    )
    out_specs = (
        P("section", None, "ctx", None),
        P("section", None, "ctx", None),
        P("section", None, "ctx", None),
    )

    def shards(query_in, key_in, value_in, forward_out, log_sum, grad_out, block_order):
        _, micro, rows, width = query_in.shape
        head = key_in.shape[3]
        heads = width // head
        group = 2 if heads % 2 == 0 else 1
        chunks = heads // group
        wide = group * head
        low, full = jnp.bfloat16, jnp.float32
        dma = pltpu.SemaphoreType.DMA
        others = WINDOW - 1
        dq, kv_out = pl.pallas_call(
            functools.partial(kernel, members, sections, block_order.shape[0]),
            out_shape=(
                pltpu.VMEM((micro, chunks, rows, wide), low),
                pltpu.VMEM((micro, 2, rows, head), low),
            ),
            in_specs=[pl.BlockSpec(memory_space=pl.ANY)] * 7,
            out_specs=[pl.BlockSpec(memory_space=pltpu.VMEM)] * 2,
            scratch_shapes=[
                pltpu.VMEM((3, micro, rows, width), low),
                pltpu.VMEM((micro, heads, rows), full),
                pltpu.VMEM((micro, WINDOW, 2, rows, head), low),
                pltpu.VMEM((WINDOW * rows, group * rows), full),
                pltpu.VMEM((chunks, rows, wide), low),
                pltpu.VMEM((micro, 2, rows, head), full),
                pltpu.VMEM((micro, others, 2, rows, head), low),
                pltpu.VMEM((micro, others, 2, rows, head), low),
                pltpu.VMEM((chunks, group * rows, head), full),
                pltpu.VMEM((WINDOW * rows, heads * rows), low),
                pltpu.VMEM((WINDOW * rows, heads * rows), low),
                pltpu.VMEM((WINDOW * rows, heads * rows), full),
                pltpu.VMEM((2, others * rows, head), full),
                pltpu.SMEM(block_order.shape, jnp.int32),
                dma, dma, dma, dma((micro,)),
                dma, dma((micro,)), dma((micro,)), dma, dma((micro,)), dma, dma, dma((chunks,)),
            ],
            compiler_params=pltpu.CompilerParams(collective_id=0, has_side_effects=True),
        )(block_order, query_in, key_in, value_in, forward_out, grad_out, log_sum)
        return pl.pallas_call(
            writer,
            out_shape=(
                jax.ShapeDtypeStruct(query_in.shape, low),
                jax.ShapeDtypeStruct(key_in.shape, low),
                jax.ShapeDtypeStruct(value_in.shape, low),
            ),
            in_specs=[pl.BlockSpec(memory_space=pltpu.VMEM)] * 2,
            out_specs=[pl.BlockSpec(memory_space=pl.ANY)] * 3,
            scratch_shapes=[dma((2,))],
        )(*(pltpu.with_memory_space_constraint(x, pltpu.VMEM) for x in (dq, kv_out)))

    return jax.shard_map(shards, mesh=mesh, in_specs=in_specs, out_specs=out_specs, check_vma=False)
```

```python
import functools
import math

import jax
import jax.numpy as jnp
from jax import lax
from jax.experimental import pallas as pl
from jax.experimental.pallas import tpu as pltpu
from jax.sharding import PartitionSpec as P

WINDOW = 3
KEEP = 2
YIELD = -1
HOLD = 1
LOG2E = math.log2(math.e)
HIDE = -1e30


def dot(a, b, dims):
    return lax.dot_general(a, b, (dims, ((), ())), preferred_element_type=jnp.float32)


def kernel(
    members, sections, blocks,
    order_hbm, q_hbm, k_hbm, v_hbm, fo_hbm, go_hbm, log_hbm,
    dq, kv_out,
    rows_in, logs, kv, bias, passed, own, part, back, dq_own, ds, pr, pf, far_sum, order,
    order_sem, rows_sem, log_sem, kv_sem,
    kv_send, k_recv, v_recv, part_send, part_recv, relay_recv, hop_send, hop_recv,
):
    _, micro, rows, width = rows_in.shape
    q, go, fo = rows_in.at[0], rows_in.at[1], rows_in.at[2]
    head = kv.shape[-1]
    chunks, _, wide = passed.shape
    group = wide // head
    span = group * rows
    factor = 1.0 / math.sqrt(head)
    me = lax.axis_index("ctx")
    sec = lax.axis_index("section")
    peer = lambda offset: {"ctx": lax.rem(me + offset + members, members)}
    below = {"section": jnp.maximum(sec - 1, 0)}
    above = {"section": jnp.minimum(sec + 1, sections - 1)}
    has_below = sec > 0
    has_above = sec < sections - 1
    first = lax.rem(me, 2) == 0

    barrier = pltpu.get_barrier_semaphore()
    near = sorted({o % members for o in range(1 - WINDOW, WINDOW)} - {0})
    for o in near:
        pl.semaphore_signal(barrier, inc=1, device_id=peer(o), device_id_type=pl.DeviceIdType.MESH)

    @pl.when(has_above)
    def _():
        pl.semaphore_signal(barrier, inc=1, device_id=above, device_id_type=pl.DeviceIdType.MESH)

    def arrived(ref, sem):
        pltpu.make_async_copy(ref, ref, sem).wait()

    for m in range(micro):
        for which, source in enumerate((k_hbm, v_hbm)):
            pltpu.make_async_copy(source.at[0, m], kv.at[m, 0, which], kv_sem.at[m]).start()
    order_load = pltpu.make_async_copy(order_hbm, order, order_sem)
    order_load.start()
    log_load = pltpu.make_async_copy(log_hbm.at[0], logs, log_sem)
    log_load.start()
    for which, source in enumerate((q_hbm, go_hbm, fo_hbm)):
        pltpu.make_async_copy(source.at[0], rows_in.at[which], rows_sem).start()

    if True:
        pl.semaphore_wait(barrier, len(near) + has_below.astype(jnp.int32))

    others = pl.ds(1, WINDOW - 1)
    far_recv = (k_recv, v_recv)

    def move_kv(m, source, which, offset, slot):
        pltpu.make_async_remote_copy(
            src_ref=kv.at[m, source, which], dst_ref=kv.at[m, slot, which],
            send_sem=kv_send, recv_sem=far_recv[which].at[m],
            device_id=peer(offset), device_id_type=pl.DeviceIdType.MESH,
        ).start()

    def send_kv(m, who):
        @pl.when(who)
        def _():
            for which in range(2):
                move_kv(m, 0, which, 2, 2)

    def take_kv(m, which):
        arrived(kv.at[m, others, which], far_recv[which].at[m])

        @pl.when(jnp.logical_not(first))
        def _():
            move_kv(m, 2, which, -1, 1)

    arrived(kv.at[0, 0], kv_sem.at[0])

    @pl.when(first)
    def _():
        for which in range(2):
            move_kv(0, 0, which, 1, 1)
    send_kv(0, jnp.logical_not(first))
    if YIELD < 0:
        send_kv(0, first)

    half = members * rows // blocks
    per = rows // half
    lane = lax.broadcasted_iota(jnp.int32, (half, rows), 1)
    down = lax.broadcasted_iota(jnp.int32, (half, rows), 0)
    q_place = lax.rem(lane, half)
    order_load.wait()
    for b in range(per):
        base = order[me * per + b] * half
        q_place = q_place + jnp.where(lane // half == b, base, 0)
    for o in range(WINDOW):
        source = lax.rem(me - o + members, members)
        for b in range(per):
            k_place = down + order[source * per + b] * half
            tile = jnp.where(k_place <= q_place, 0.0, HIDE)
            for g in range(group):
                bias[pl.ds(o * rows + b * half, half), pl.ds(g * rows, rows)] = tile

    @pl.when(jnp.logical_not(has_above))
    def _():
        passed[...] = jnp.zeros_like(passed)

    ones = jnp.ones((8, head), jnp.bfloat16)
    near_rows = pl.ds(rows, (WINDOW - 1) * rows)
    own_rows = pl.ds(0, rows)

    def split(block):
        return jnp.concatenate([block[:, g * head:(g + 1) * head] for g in range(group)], axis=0)

    def stack(block):
        return jnp.concatenate([block[:, h * head:(h + 1) * head] for h in range(width // head)], axis=0)

    def cols(c):
        return pl.ds(c * wide, wide)

    def lanes(c):
        return pl.ds(c * span, span)

    def queries(m, c):
        return split(q[m, :, cols(c)])

    def row_dots(m, c, upstream):
        product = upstream.astype(jnp.float32) * split(fo[m, :, cols(c)]).astype(jnp.float32)
        high = product.astype(jnp.bfloat16)
        low = (product - high.astype(jnp.float32)).astype(jnp.bfloat16)
        return (dot(ones, high, ((1,), (1,))) + dot(ones, low, ((1,), (1,))))[0:1]

    def probs_of(m, c, keys, where):
        log_row = jnp.concatenate(
            [logs[m, pl.ds(c * group + g, 1), :] for g in range(group)], axis=1
        ) * LOG2E
        scores = dot(keys, queries(m, c), ((1,), (1,)))
        return jnp.exp2(scores * (factor * LOG2E) - log_row + bias[where])

    def far(m, which):
        return jnp.concatenate([kv[m, o, which] for o in range(1, WINDOW)], axis=0)

    def grads_of(probs, values, upstream, row_dot):
        return (probs * (dot(values, upstream, ((1,), (1,))) - row_dot)).astype(jnp.bfloat16)

    def put_dq(m, c, grad_query):
        for g in range(group):
            dq[m, c, :, pl.ds(g * head, head)] = grad_query[g * rows:(g + 1) * rows].astype(jnp.bfloat16)

    def hop(c):
        return pltpu.make_async_remote_copy(
            src_ref=dq.at[0, c], dst_ref=passed.at[c],
            send_sem=hop_send, recv_sem=hop_recv.at[c],
            device_id=below, device_id_type=pl.DeviceIdType.MESH,
        )

    def send_piece(m, o, which, offset, recv_sem):
        pltpu.make_async_remote_copy(
            src_ref=part.at[m, o - 1, which], dst_ref=back.at[m, o - 1, which],
            send_sem=part_send, recv_sem=recv_sem,
            device_id=peer(offset), device_id_type=pl.DeviceIdType.MESH,
        ).start()

    def send_parts(m, dk, dv):
        for o in range(WINDOW - 1, 0, -1):
            for which, total in enumerate((dk, dv)):
                part[m, o - 1, which] = total[(o - 1) * rows:o * rows].astype(jnp.bfloat16)
                send_piece(m, o, which, -o, part_recv.at[m])

    def finish(m):
        if m < micro - 1:
            arrived(back.at[m], part_recv.at[m])
        else:
            @pl.when(first)
            def _():
                arrived(back.at[m], part_recv.at[m])

            @pl.when(jnp.logical_not(first))
            def _():
                arrived(back.at[m, 1], part_recv.at[m])
        for which in range(2):
            total = own[m, which] + back[m, 1, which].astype(jnp.float32)
            beside = back[m, 0, which].astype(jnp.float32)
            if m == micro - 1:
                beside = jnp.where(first, beside, 0.0)
            kv_out[m, which] = (total + beside).astype(jnp.bfloat16)

    if True:
        log_load.wait()
        arrived(rows_in, rows_sem)
    keys, values = kv[0, 0, 0], kv[0, 0, 1]
    row_dot = []
    if True:
        for c in range(chunks):
            upstream = split(go[0, :, cols(c)])
            row_dot.append(row_dots(0, c, upstream))
            probs = probs_of(0, c, keys, own_rows)
            grads = grads_of(probs, values, upstream, row_dot[c])
            pr[own_rows, lanes(c)] = probs.astype(jnp.bfloat16)
            ds[own_rows, lanes(c)] = grads
            dq_own[c] = dot(grads, keys, ((0,), (0,)))
            if c == YIELD:
                send_kv(0, first)

    if True:
        take_kv(0, 0)
    keys = far(0, 0)
    if True:
        for c in range(chunks):
            pf[near_rows, lanes(c)] = probs_of(0, c, keys, near_rows)
    if True:
        take_kv(0, 1)
    for m in range(1, micro):
        arrived(kv.at[m, 0], kv_sem.at[m])
        for which in range(2):
            move_kv(m, 0, which, 2, 2)

        @pl.when(first)
        def _(m=m):
            for which in range(2):
                move_kv(m, 0, which, 1, 1)
    values = far(0, 1)
    for c in range(chunks):
        if True:
            upstream = split(go[0, :, cols(c)])
            probs = pf[near_rows, lanes(c)]
            grads = grads_of(probs, values, upstream, row_dot[c])
            ds[near_rows, lanes(c)] = grads
            put_dq(0, c, (dq_own[c] + dot(grads, keys, ((0,), (0,)))) * factor)

            @pl.when(has_below if c < KEEP else jnp.logical_and(has_below, first))
            def _(c=c):
                hop(c).start()

            pr[near_rows, lanes(c)] = probs.astype(jnp.bfloat16)

    if True:
        all_queries, all_upstream = stack(q[0]), stack(go[0])
        dk = dot(ds[...], all_queries, ((1,), (0,))) * factor
        dv = dot(pr[...], all_upstream, ((1,), (0,)))
        send_parts(0, dk[rows:], dv[rows:])
        own[0, 0] = dk[:rows]
        own[0, 1] = dv[:rows]

    for m in range(1, micro):
        if True:
            for which in range(2):
                take_kv(m, which)
        keys = jnp.concatenate([kv[m, o, 0] for o in range(WINDOW)], axis=0)
        if True:
            for c in range(chunks):
                pf[:, lanes(c)] = probs_of(m, c, keys, pl.ds(0, WINDOW * rows))

        far_values, own_values = far(m, 1), kv[m, 0, 1]
        all_queries = stack(q[m])
        ready = (chunks - 1) * span
        dots, ups = [], []

        def send_held(who):
            @pl.when(jnp.logical_and(has_below, jnp.logical_and(jnp.logical_not(first), who)))
            def _():
                for held in range(KEEP, chunks):
                    hop(held).start()

        def sum_far(start, stop):
            early = pl.ds(start * span, (stop - start) * span)
            for which, (left, right) in enumerate((
                (ds, all_queries[start * span:stop * span]),
                (pr, jnp.concatenate(ups[start:stop], axis=0)),
            )):
                total = dot(left[near_rows, early], right, ((1,), (0,)))
                far_sum[which] = total if start == 0 else far_sum[which] + total

        for c in range(chunks):
            if c == HOLD + 1:
                if True:
                    sum_far(0, c)
                if m == 1:
                    send_held(has_above)
            if c == chunks - 1:
                if True:
                    sum_far(HOLD + 1, c)
                if m == 1:
                    send_held(jnp.logical_not(has_above))
            if m == 1:
                @pl.when(has_above)
                def _(c=c):
                    if True:
                        hop(c).wait_recv()
            if True:
                upstream = split((
                    go[m, :, cols(c)].astype(jnp.float32) + passed[c].astype(jnp.float32)
                ).astype(jnp.bfloat16))
                ups.append(upstream)
                dots.append(row_dots(m, c, upstream))
                probs = pf[near_rows, lanes(c)]
                grads = grads_of(probs, far_values, upstream, dots[c])
                ds[near_rows, lanes(c)] = grads
                probs = probs.astype(jnp.bfloat16)
                if c < chunks - 1:
                    pr[near_rows, lanes(c)] = probs
                else:
                    sums = [None, None]
                    sums[1] = far_sum[1] + dot(probs, upstream, ((1,), (0,)))
                    sums[0] = (far_sum[0] + dot(grads, all_queries[ready:], ((1,), (0,)))) * factor
                    for which in (1, 0):
                        total = sums[which]
                        part[m, 0, which] = total[:rows].astype(jnp.bfloat16)

                        @pl.when(first)
                        def _(which=which, total=total):
                            send_piece(m, 1, which, 1, relay_recv.at[which])
                            part[m, 1, which] = total[rows:].astype(jnp.bfloat16)
                            send_piece(m, 2, which, -2, part_recv.at[m])

                        @pl.when(jnp.logical_not(first))
                        def _(which=which, total=total):
                            send_piece(m, 1, which, -1, part_recv.at[m])
                            arrived(back.at[m, 0, which], relay_recv.at[which])
                            both = total[rows:] + back[m, 0, which].astype(jnp.float32)
                            part[m, 1, which] = both.astype(jnp.bfloat16)
                            send_piece(m, 2, which, -2, part_recv.at[m])
        if True:
            for c in range(chunks):
                probs = pf[own_rows, lanes(c)]
                ds[own_rows, lanes(c)] = grads_of(probs, own_values, ups[c], dots[c])
                pr[own_rows, lanes(c)] = probs.astype(jnp.bfloat16)
                put_dq(m, c, dot(ds[:, lanes(c)], keys, ((0,), (0,))) * factor)
            own[m, 0] = dot(ds[own_rows, :], all_queries, ((1,), (0,))) * factor
            own[m, 1] = dot(pr[own_rows, :], jnp.concatenate(ups, axis=0), ((1,), (0,)))

    for m in range(micro):
        if True:
            finish(m)
    arrived(kv.at[:, others], kv_send)
    arrived(part, part_send)

    @pl.when(has_below)
    def _():
        arrived(passed, hop_send)


def writer(dq, kv_out, dq_hbm, dk_hbm, dv_hbm, sem):
    micro, chunks, _, wide = dq.shape
    for m in range(micro):
        for c in range(chunks):
            pltpu.make_async_copy(
                dq.at[m, c], dq_hbm.at[0, m, :, pl.ds(c * wide, wide)], sem.at[0]
            ).start()
        for which, target in enumerate((dk_hbm, dv_hbm)):
            pltpu.make_async_copy(kv_out.at[m, which], target.at[0, m], sem.at[1]).start()
    pltpu.make_async_copy(dq, dq, sem.at[0]).wait()
    pltpu.make_async_copy(kv_out, kv_out, sem.at[1]).wait()


def solution(mesh):
    members = mesh.shape["ctx"]
    sections = mesh.shape["section"]
    in_specs = (
        P("section", None, "ctx", None),
        P("section", None, "ctx", None),
        P("section", None, "ctx", None),
        P("section", None, "ctx", None),
        P("section", None, None, "ctx"),
        P("section", None, "ctx", None),
        P(),
    )
    out_specs = (
        P("section", None, "ctx", None),
        P("section", None, "ctx", None),
        P("section", None, "ctx", None),
    )

    def shards(query_in, key_in, value_in, forward_out, log_sum, grad_out, block_order):
        _, micro, rows, width = query_in.shape
        head = key_in.shape[3]
        heads = width // head
        group = 2 if heads % 2 == 0 else 1
        chunks = heads // group
        wide = group * head
        low, full = jnp.bfloat16, jnp.float32
        dma = pltpu.SemaphoreType.DMA
        others = WINDOW - 1
        dq, kv_out = pl.pallas_call(
            functools.partial(kernel, members, sections, block_order.shape[0]),
            out_shape=(
                pltpu.VMEM((micro, chunks, rows, wide), low),
                pltpu.VMEM((micro, 2, rows, head), low),
            ),
            in_specs=[pl.BlockSpec(memory_space=pl.ANY)] * 7,
            out_specs=[pl.BlockSpec(memory_space=pltpu.VMEM)] * 2,
            scratch_shapes=[
                pltpu.VMEM((3, micro, rows, width), low),
                pltpu.VMEM((micro, heads, rows), full),
                pltpu.VMEM((micro, WINDOW, 2, rows, head), low),
                pltpu.VMEM((WINDOW * rows, group * rows), full),
                pltpu.VMEM((chunks, rows, wide), low),
                pltpu.VMEM((micro, 2, rows, head), full),
                pltpu.VMEM((micro, others, 2, rows, head), low),
                pltpu.VMEM((micro, others, 2, rows, head), low),
                pltpu.VMEM((chunks, group * rows, head), full),
                pltpu.VMEM((WINDOW * rows, heads * rows), low),
                pltpu.VMEM((WINDOW * rows, heads * rows), low),
                pltpu.VMEM((WINDOW * rows, heads * rows), full),
                pltpu.VMEM((2, others * rows, head), full),
                pltpu.SMEM(block_order.shape, jnp.int32),
                dma, dma, dma, dma((micro,)),
                dma, dma((micro,)), dma((micro,)), dma, dma((micro,)), dma((2,)), dma, dma((chunks,)),
            ],
            compiler_params=pltpu.CompilerParams(collective_id=0, has_side_effects=True),
        )(block_order, query_in, key_in, value_in, forward_out, grad_out, log_sum)
        return pl.pallas_call(
            writer,
            out_shape=(
                jax.ShapeDtypeStruct(query_in.shape, low),
                jax.ShapeDtypeStruct(key_in.shape, low),
                jax.ShapeDtypeStruct(value_in.shape, low),
            ),
            in_specs=[pl.BlockSpec(memory_space=pltpu.VMEM)] * 2,
            out_specs=[pl.BlockSpec(memory_space=pl.ANY)] * 3,
            scratch_shapes=[dma((2,))],
        )(*(pltpu.with_memory_space_constraint(x, pltpu.VMEM) for x in (dq, kv_out)))

    return jax.shard_map(shards, mesh=mesh, in_specs=in_specs, out_specs=out_specs, check_vma=False)
```

```python
import functools
import math

import jax
import jax.numpy as jnp
from jax import lax
from jax.experimental import pallas as pl
from jax.experimental.pallas import tpu as pltpu
from jax.sharding import PartitionSpec as P

WINDOW = 3
LOG2E = math.log2(math.e)
HIDE = -1e30


def dot(a, b, dims):
    return lax.dot_general(a, b, (dims, ((), ())), preferred_element_type=jnp.float32)


def plan_of(heads, group):
    return [(h, group) for h in range(0, heads, group)]


def kernel(
    members, sections, blocks,
    order_hbm, q_hbm, k_hbm, v_hbm, fo_hbm, go_hbm, log_hbm,
    dq, kv_out,
    rows_in, logs, kv, bias, passed, own, part, back, dq_own, ds, pr, pf, ups, far_sum, order,
    order_sem, rows_sem, log_sem, kv_sem,
    kv_send, k_recv, v_recv, part_send, part_recv, relay_recv, hop_send, hop_recv,
):
    _, micro, rows, width = rows_in.shape
    q, go, fo = rows_in.at[0], rows_in.at[1], rows_in.at[2]
    head = kv.shape[-1]
    heads = width // head
    group = bias.shape[1] // rows
    pairs = [(h, group) for h in range(0, heads, group)]
    plan = plan_of(heads, group)
    early = [h for h, _ in plan].index(heads // 2)
    factor = 1.0 / math.sqrt(head)
    me = lax.axis_index("ctx")
    sec = lax.axis_index("section")
    peer = lambda offset: {"ctx": lax.rem(me + offset + members, members)}
    below = {"section": jnp.maximum(sec - 1, 0)}
    above = {"section": jnp.minimum(sec + 1, sections - 1)}
    has_below = sec > 0
    has_above = sec < sections - 1
    first = lax.rem(me, 2) == 0
    yields = lax.rem(me, 4) == 0

    barrier = pltpu.get_barrier_semaphore()
    near = sorted({o % members for o in range(1 - WINDOW, WINDOW)} - {0})
    for o in near:
        pl.semaphore_signal(barrier, inc=1, device_id=peer(o), device_id_type=pl.DeviceIdType.MESH)

    @pl.when(has_above)
    def _():
        pl.semaphore_signal(barrier, inc=1, device_id=above, device_id_type=pl.DeviceIdType.MESH)

    def arrived(ref, sem):
        pltpu.make_async_copy(ref, ref, sem).wait()

    for m in range(micro):
        for which, source in enumerate((k_hbm, v_hbm)):
            pltpu.make_async_copy(source.at[0, m], kv.at[m, 0, which], kv_sem.at[m]).start()
    order_load = pltpu.make_async_copy(order_hbm, order, order_sem)
    order_load.start()
    log_load = pltpu.make_async_copy(log_hbm.at[0], logs, log_sem)
    log_load.start()
    for which, source in enumerate((q_hbm, go_hbm, fo_hbm)):
        pltpu.make_async_copy(source.at[0], rows_in.at[which], rows_sem).start()

    if True:
        pl.semaphore_wait(barrier, len(near) + has_below.astype(jnp.int32))

    others = pl.ds(1, WINDOW - 1)
    far_recv = (k_recv, v_recv)

    def move_kv(m, source, which, offset, slot):
        pltpu.make_async_remote_copy(
            src_ref=kv.at[m, source, which], dst_ref=kv.at[m, slot, which],
            send_sem=kv_send, recv_sem=far_recv[which].at[m],
            device_id=peer(offset), device_id_type=pl.DeviceIdType.MESH,
        ).start()

    def send_kv(m, which, who):
        @pl.when(who)
        def _():
            move_kv(m, 0, which, 2, 2)

    def take_kv(m, which):
        arrived(kv.at[m, others, which], far_recv[which].at[m])

        @pl.when(jnp.logical_not(first))
        def _():
            move_kv(m, 2, which, -1, 1)

    arrived(kv.at[0, 0], kv_sem.at[0])

    @pl.when(first)
    def _():
        for which in range(2):
            move_kv(0, 0, which, 1, 1)
    move_kv(0, 0, 0, 2, 2)
    send_kv(0, 1, jnp.logical_not(yields))

    half = members * rows // blocks
    per = rows // half
    lane = lax.broadcasted_iota(jnp.int32, (half, rows), 1)
    down = lax.broadcasted_iota(jnp.int32, (half, rows), 0)
    q_place = lax.rem(lane, half)
    order_load.wait()
    for b in range(per):
        base = order[me * per + b] * half
        q_place = q_place + jnp.where(lane // half == b, base, 0)
    for o in range(WINDOW):
        source = lax.rem(me - o + members, members)
        for b in range(per):
            k_place = down + order[source * per + b] * half
            tile = jnp.where(k_place <= q_place, 0.0, HIDE)
            for g in range(group):
                bias[pl.ds(o * rows + b * half, half), pl.ds(g * rows, rows)] = tile

    @pl.when(jnp.logical_not(has_above))
    def _():
        passed[...] = jnp.zeros_like(passed)

    ones = jnp.ones((8, head), jnp.bfloat16)
    near_rows = pl.ds(rows, (WINDOW - 1) * rows)
    own_rows = pl.ds(0, rows)

    def split(block):
        return jnp.concatenate([block[:, i:i + head] for i in range(0, block.shape[1], head)], axis=0)

    def cols(h, n):
        return pl.ds(h * head, n * head)

    def lanes(h, n):
        return pl.ds(h * rows, n * rows)

    def row_dots(upstream, saved):
        product = upstream.astype(jnp.float32) * saved.astype(jnp.float32)
        high = product.astype(jnp.bfloat16)
        low = (product - high.astype(jnp.float32)).astype(jnp.bfloat16)
        total = (dot(ones, high, ((1,), (1,))) + dot(ones, low, ((1,), (1,))))[0:1]
        return [total[:, i:i + rows] for i in range(0, total.shape[1], rows)]

    def joined(row_dot, h, n):
        return jnp.concatenate(row_dot[h:h + n], axis=1)

    def probs_of(m, h, n, keys, where):
        log_row = jnp.concatenate([logs[m, pl.ds(g, 1), :] for g in range(h, h + n)], axis=1) * LOG2E
        scores = dot(keys, split(q[m, :, cols(h, n)]), ((1,), (1,)))
        return jnp.exp2(scores * (factor * LOG2E) - log_row + bias[where, pl.ds(0, n * rows)])

    def far(m, which):
        return jnp.concatenate([kv[m, o, which] for o in range(1, WINDOW)], axis=0)

    def grads_of(probs, values, upstream, row_dot):
        return (probs * (dot(values, upstream, ((1,), (1,))) - row_dot)).astype(jnp.bfloat16)

    def put_dq(m, h, n, grad_query):
        for g in range(n):
            dq[m, h + g] = grad_query[g * rows:(g + 1) * rows].astype(jnp.bfloat16)

    def hop(c):
        part_of = pl.ds(*plan[c])
        return pltpu.make_async_remote_copy(
            src_ref=dq.at[0, part_of], dst_ref=passed.at[part_of],
            send_sem=hop_send, recv_sem=hop_recv.at[c],
            device_id=below, device_id_type=pl.DeviceIdType.MESH,
        )

    def send_piece(m, o, which, offset, recv_sem):
        pltpu.make_async_remote_copy(
            src_ref=part.at[m, o - 1, which], dst_ref=back.at[m, o - 1, which],
            send_sem=part_send, recv_sem=recv_sem,
            device_id=peer(offset), device_id_type=pl.DeviceIdType.MESH,
        ).start()

    def send_parts(m, dk, dv):
        for o in range(WINDOW - 1, 0, -1):
            for which, total in enumerate((dk, dv)):
                part[m, o - 1, which] = total[(o - 1) * rows:o * rows].astype(jnp.bfloat16)
                send_piece(m, o, which, -o, part_recv.at[m])

    def finish(m):
        if m < micro - 1:
            arrived(back.at[m], part_recv.at[m])
        else:
            @pl.when(first)
            def _():
                arrived(back.at[m], part_recv.at[m])

            @pl.when(jnp.logical_not(first))
            def _():
                arrived(back.at[m, 1], part_recv.at[m])
        for which in range(2):
            total = own[m, which] + back[m, 1, which].astype(jnp.float32)
            beside = back[m, 0, which].astype(jnp.float32)
            if m == micro - 1:
                beside = jnp.where(first, beside, 0.0)
            kv_out[m, which] = (total + beside).astype(jnp.bfloat16)

    if True:
        log_load.wait()
        arrived(rows_in, rows_sem)
    keys, values = kv[0, 0, 0], kv[0, 0, 1]
    row_dot = []
    if True:
        for h, n in pairs:
            upstream = split(go[0, :, cols(h, n)])
            row_dot += row_dots(upstream, split(fo[0, :, cols(h, n)]))
            probs = probs_of(0, h, n, keys, own_rows)
            grads = grads_of(probs, values, upstream, joined(row_dot, h, n))
            pr[own_rows, lanes(h, n)] = probs.astype(jnp.bfloat16)
            ds[own_rows, lanes(h, n)] = grads
            dq_own[lanes(h, n), :] = dot(grads, keys, ((0,), (0,)))
            if h == 0:
                send_kv(0, 1, yields)

    if True:
        take_kv(0, 0)
    keys = far(0, 0)
    if True:
        for h, n in plan[:1]:
            pf[near_rows, lanes(h, n)] = probs_of(0, h, n, keys, near_rows)
    if True:
        take_kv(0, 1)
    for m in range(1, micro):
        arrived(kv.at[m, 0], kv_sem.at[m])
        for which in range(2):
            move_kv(m, 0, which, 2, 2)

        @pl.when(first)
        def _(m=m):
            for which in range(2):
                move_kv(m, 0, which, 1, 1)
    values = far(0, 1)
    for c, (h, n) in enumerate(plan):
        if True:
            upstream = split(go[0, :, cols(h, n)])
            probs = pf[near_rows, lanes(h, n)] if c < 1 else probs_of(0, h, n, keys, near_rows)
            grads = grads_of(probs, values, upstream, joined(row_dot, h, n))
            ds[near_rows, lanes(h, n)] = grads
            put_dq(0, h, n, (dq_own[lanes(h, n), :] + dot(grads, keys, ((0,), (0,)))) * factor)

            @pl.when(has_below if c < early else jnp.logical_and(has_below, first))
            def _(c=c):
                hop(c).start()

            pr[near_rows, lanes(h, n)] = probs.astype(jnp.bfloat16)

    if True:
        all_queries, all_upstream = split(q[0]), split(go[0])
        dk = dot(ds[...], all_queries, ((1,), (0,))) * factor
        dv = dot(pr[...], all_upstream, ((1,), (0,)))
        send_parts(0, dk[rows:], dv[rows:])
        own[0, 0] = dk[:rows]
        own[0, 1] = dv[:rows]

    for m in range(1, micro):
        if True:
            for which in range(2):
                take_kv(m, which)
        keys = jnp.concatenate([kv[m, o, 0] for o in range(WINDOW)], axis=0)
        if True:
            for h, n in pairs:
                pf[:, lanes(h, n)] = probs_of(m, h, n, keys, pl.ds(0, WINDOW * rows))

        far_values, own_values = far(m, 1), kv[m, 0, 1]
        all_queries = split(q[m])
        row_dot = []

        def send_held(who):
            @pl.when(jnp.logical_and(has_below, jnp.logical_and(jnp.logical_not(first), who)))
            def _():
                for held in range(early, len(plan)):
                    hop(held).start()

        def key_sum(h, n):
            return dot(ds[near_rows, lanes(h, n)], all_queries[h * rows:(h + n) * rows], ((1,), (0,)))

        def value_sum(h, n):
            return dot(pr[near_rows, lanes(h, n)], ups[lanes(h, n), :], ((1,), (0,)))

        def send_sum(which, total):
            part[m, 0, which] = total[:rows].astype(jnp.bfloat16)

            @pl.when(first)
            def _():
                send_piece(m, 1, which, 1, relay_recv.at[which])
                part[m, 1, which] = total[rows:].astype(jnp.bfloat16)
                send_piece(m, 2, which, -2, part_recv.at[m])

            @pl.when(jnp.logical_not(first))
            def _():
                send_piece(m, 1, which, -1, part_recv.at[m])
                arrived(back.at[m, 0, which], relay_recv.at[which])
                both = total[rows:] + back[m, 0, which].astype(jnp.float32)
                part[m, 1, which] = both.astype(jnp.bfloat16)
                send_piece(m, 2, which, -2, part_recv.at[m])

        def sum_far(h, n):
            for which, total in enumerate((key_sum(h, n), value_sum(h, n))):
                far_sum[which] = total if h == 0 else far_sum[which] + total

        for c, (h, n) in enumerate(plan):
            if c == early:
                if True:
                    sum_far(0, h)
                if m == 1:
                    send_held(has_above)
            if c == len(plan) - 1:
                if True:
                    sum_far(plan[early][0], h - plan[early][0])
                if m == 1:
                    send_held(jnp.logical_not(has_above))
            if m == 1:
                @pl.when(has_above)
                def _(c=c):
                    if True:
                        hop(c).wait_recv()
            if True:
                upstream = (
                    split(go[m, :, cols(h, n)]).astype(jnp.float32)
                    + passed[h:h + n].reshape(n * rows, head).astype(jnp.float32)
                ).astype(jnp.bfloat16)
                ups[lanes(h, n), :] = upstream
                row_dot += row_dots(upstream, split(fo[m, :, cols(h, n)]))
                probs = pf[near_rows, lanes(h, n)]
                pr[near_rows, lanes(h, n)] = probs.astype(jnp.bfloat16)
                grad_probs = dot(far_values, upstream, ((1,), (1,))) - joined(row_dot, h, n)
                if c == len(plan) - 1:
                    send_sum(1, far_sum[1] + value_sum(h, n))
                ds[near_rows, lanes(h, n)] = (probs * grad_probs).astype(jnp.bfloat16)
                if c == len(plan) - 1:
                    send_sum(0, (far_sum[0] + key_sum(h, n)) * factor)
        if True:
            for h, n in pairs:
                at = lanes(h, n)
                probs = pf[own_rows, at]
                ds[own_rows, at] = grads_of(probs, own_values, ups[at, :], joined(row_dot, h, n))
                pr[own_rows, at] = probs.astype(jnp.bfloat16)
                put_dq(m, h, n, dot(ds[:, at], keys, ((0,), (0,))) * factor)
            own[m, 0] = dot(ds[own_rows, :], all_queries, ((1,), (0,))) * factor
            own[m, 1] = dot(pr[own_rows, :], ups[...], ((1,), (0,)))

    for m in range(micro):
        if True:
            finish(m)
    arrived(kv.at[:, others], kv_send)
    arrived(part, part_send)

    @pl.when(has_below)
    def _():
        arrived(passed, hop_send)


def writer(dq, kv_out, dq_hbm, dk_hbm, dv_hbm, sem):
    micro, heads, _, head = dq.shape
    for m in range(micro):
        for h in range(heads):
            pltpu.make_async_copy(
                dq.at[m, h], dq_hbm.at[0, m, :, pl.ds(h * head, head)], sem.at[0]
            ).start()
        for which, target in enumerate((dk_hbm, dv_hbm)):
            pltpu.make_async_copy(kv_out.at[m, which], target.at[0, m], sem.at[1]).start()
    pltpu.make_async_copy(dq, dq, sem.at[0]).wait()
    pltpu.make_async_copy(kv_out, kv_out, sem.at[1]).wait()


def solution(mesh):
    members = mesh.shape["ctx"]
    sections = mesh.shape["section"]
    in_specs = (
        P("section", None, "ctx", None),
        P("section", None, "ctx", None),
        P("section", None, "ctx", None),
        P("section", None, "ctx", None),
        P("section", None, None, "ctx"),
        P("section", None, "ctx", None),
        P(),
    )
    out_specs = (
        P("section", None, "ctx", None),
        P("section", None, "ctx", None),
        P("section", None, "ctx", None),
    )

    def shards(query_in, key_in, value_in, forward_out, log_sum, grad_out, block_order):
        _, micro, rows, width = query_in.shape
        head = key_in.shape[3]
        heads = width // head
        group = 2 if heads % 2 == 0 else 1
        low, full = jnp.bfloat16, jnp.float32
        dma = pltpu.SemaphoreType.DMA
        others = WINDOW - 1
        dq, kv_out = pl.pallas_call(
            functools.partial(kernel, members, sections, block_order.shape[0]),
            out_shape=(
                pltpu.VMEM((micro, heads, rows, head), low),
                pltpu.VMEM((micro, 2, rows, head), low),
            ),
            in_specs=[pl.BlockSpec(memory_space=pl.ANY)] * 7,
            out_specs=[pl.BlockSpec(memory_space=pltpu.VMEM)] * 2,
            scratch_shapes=[
                pltpu.VMEM((3, micro, rows, width), low),
                pltpu.VMEM((micro, heads, rows), full),
                pltpu.VMEM((micro, WINDOW, 2, rows, head), low),
                pltpu.VMEM((WINDOW * rows, group * rows), full),
                pltpu.VMEM((heads, rows, head), low),
                pltpu.VMEM((micro, 2, rows, head), full),
                pltpu.VMEM((micro, others, 2, rows, head), low),
                pltpu.VMEM((micro, others, 2, rows, head), low),
                pltpu.VMEM((heads * rows, head), full),
                pltpu.VMEM((WINDOW * rows, heads * rows), low),
                pltpu.VMEM((WINDOW * rows, heads * rows), low),
                pltpu.VMEM((WINDOW * rows, heads * rows), full),
                pltpu.VMEM((heads * rows, head), low),
                pltpu.VMEM((2, others * rows, head), full),
                pltpu.SMEM(block_order.shape, jnp.int32),
                dma, dma, dma, dma((micro,)),
                dma, dma((micro,)), dma((micro,)), dma, dma((micro,)), dma((2,)), dma, dma((len(plan_of(heads, group)),)),
            ],
            compiler_params=pltpu.CompilerParams(collective_id=0, has_side_effects=True),
        )(block_order, query_in, key_in, value_in, forward_out, grad_out, log_sum)
        return pl.pallas_call(
            writer,
            out_shape=(
                jax.ShapeDtypeStruct(query_in.shape, low),
                jax.ShapeDtypeStruct(key_in.shape, low),
                jax.ShapeDtypeStruct(value_in.shape, low),
            ),
            in_specs=[pl.BlockSpec(memory_space=pltpu.VMEM)] * 2,
            out_specs=[pl.BlockSpec(memory_space=pl.ANY)] * 3,
            scratch_shapes=[dma((2,))],
        )(*(pltpu.with_memory_space_constraint(x, pltpu.VMEM) for x in (dq, kv_out)))

    return jax.shard_map(shards, mesh=mesh, in_specs=in_specs, out_specs=out_specs, check_vma=False)
```

```python
import functools
import math

import jax
import jax.numpy as jnp
from jax import lax
from jax.experimental import pallas as pl
from jax.experimental.pallas import tpu as pltpu
from jax.sharding import PartitionSpec as P

WINDOW = 3
DONE = 1
LOG2E = math.log2(math.e)
HIDE = -1e30


def dot(a, b, dims):
    return lax.dot_general(a, b, (dims, ((), ())), preferred_element_type=jnp.float32)


def plan_of(heads, group):
    return [(h, group) for h in range(0, heads, group)]


def kernel(
    members, sections, blocks,
    order_hbm, q_hbm, k_hbm, v_hbm, fo_hbm, go_hbm, log_hbm,
    dq, kv_out,
    rows_in, logs, kv, bias, passed, own, part, back, dq_own, ds, pr, pf, ups, far_sum, order,
    order_sem, rows_sem, log_sem, kv_sem,
    kv_send, k_recv, v_recv, part_send, part_recv, relay_recv, hop_send, hop_recv,
):
    _, micro, rows, width = rows_in.shape
    q, go, fo = rows_in.at[0], rows_in.at[1], rows_in.at[2]
    head = kv.shape[-1]
    heads = width // head
    group = bias.shape[1] // rows
    pairs = [(h, group) for h in range(0, heads, group)]
    plan = plan_of(heads, group)
    early = [h for h, _ in plan].index(heads // 2)
    factor = 1.0 / math.sqrt(head)
    me = lax.axis_index("ctx")
    sec = lax.axis_index("section")
    peer = lambda offset: {"ctx": lax.rem(me + offset + members, members)}
    below = {"section": jnp.maximum(sec - 1, 0)}
    above = {"section": jnp.minimum(sec + 1, sections - 1)}
    has_below = sec > 0
    has_above = sec < sections - 1
    first = lax.rem(me, 2) == 0
    yields = lax.rem(me, 4) == 0

    barrier = pltpu.get_barrier_semaphore()
    near = sorted({o % members for o in range(1 - WINDOW, WINDOW)} - {0})
    for o in near:
        pl.semaphore_signal(barrier, inc=1, device_id=peer(o), device_id_type=pl.DeviceIdType.MESH)

    @pl.when(has_above)
    def _():
        pl.semaphore_signal(barrier, inc=1, device_id=above, device_id_type=pl.DeviceIdType.MESH)

    def arrived(ref, sem):
        pltpu.make_async_copy(ref, ref, sem).wait()

    for m in range(micro):
        for which, source in enumerate((k_hbm, v_hbm)):
            pltpu.make_async_copy(source.at[0, m], kv.at[m, 0, which], kv_sem.at[m]).start()
    order_load = pltpu.make_async_copy(order_hbm, order, order_sem)
    order_load.start()
    log_load = pltpu.make_async_copy(log_hbm.at[0], logs, log_sem)
    log_load.start()
    for which, source in enumerate((q_hbm, go_hbm, fo_hbm)):
        pltpu.make_async_copy(source.at[0], rows_in.at[which], rows_sem).start()

    pl.semaphore_wait(barrier, len(near) + has_below.astype(jnp.int32))

    others = pl.ds(1, WINDOW - 1)
    far_recv = (k_recv, v_recv)

    def move_kv(m, source, which, offset, slot):
        pltpu.make_async_remote_copy(
            src_ref=kv.at[m, source, which], dst_ref=kv.at[m, slot, which],
            send_sem=kv_send, recv_sem=far_recv[which].at[m],
            device_id=peer(offset), device_id_type=pl.DeviceIdType.MESH,
        ).start()

    def send_kv(m, which, who):
        @pl.when(who)
        def _():
            move_kv(m, 0, which, 2, 2)

    def take_kv(m, which):
        arrived(kv.at[m, others, which], far_recv[which].at[m])

        @pl.when(jnp.logical_not(first))
        def _():
            move_kv(m, 2, which, -1, 1)

    arrived(kv.at[0, 0], kv_sem.at[0])

    @pl.when(first)
    def _():
        for which in range(2):
            move_kv(0, 0, which, 1, 1)
    move_kv(0, 0, 0, 2, 2)
    send_kv(0, 1, jnp.logical_not(yields))

    half = members * rows // blocks
    per = rows // half
    lane = lax.broadcasted_iota(jnp.int32, (half, rows), 1)
    down = lax.broadcasted_iota(jnp.int32, (half, rows), 0)
    q_place = lax.rem(lane, half)
    order_load.wait()
    for b in range(per):
        base = order[me * per + b] * half
        q_place = q_place + jnp.where(lane // half == b, base, 0)
    for o in range(WINDOW):
        source = lax.rem(me - o + members, members)
        for b in range(per):
            k_place = down + order[source * per + b] * half
            tile = jnp.where(k_place <= q_place, 0.0, HIDE)
            for g in range(group):
                bias[pl.ds(o * rows + b * half, half), pl.ds(g * rows, rows)] = tile

    @pl.when(jnp.logical_not(has_above))
    def _():
        passed[...] = jnp.zeros_like(passed)

    ones = jnp.ones((8, head), jnp.bfloat16)
    near_rows = pl.ds(rows, (WINDOW - 1) * rows)
    own_rows = pl.ds(0, rows)

    def split(block):
        return jnp.concatenate([block[:, i:i + head] for i in range(0, block.shape[1], head)], axis=0)

    def cols(h, n):
        return pl.ds(h * head, n * head)

    def lanes(h, n):
        return pl.ds(h * rows, n * rows)

    def row_dots(upstream, saved):
        product = upstream.astype(jnp.float32) * saved.astype(jnp.float32)
        high = product.astype(jnp.bfloat16)
        low = (product - high.astype(jnp.float32)).astype(jnp.bfloat16)
        total = (dot(ones, high, ((1,), (1,))) + dot(ones, low, ((1,), (1,))))[0:1]
        return [total[:, i:i + rows] for i in range(0, total.shape[1], rows)]

    def joined(row_dot, h, n):
        return jnp.concatenate(row_dot[h:h + n], axis=1)

    def probs_of(m, h, n, keys, where):
        log_row = jnp.concatenate([logs[m, pl.ds(g, 1), :] for g in range(h, h + n)], axis=1) * LOG2E
        scores = dot(keys, split(q[m, :, cols(h, n)]), ((1,), (1,)))
        return jnp.exp2(scores * (factor * LOG2E) - log_row + bias[where, pl.ds(0, n * rows)])

    def far(m, which):
        return jnp.concatenate([kv[m, o, which] for o in range(1, WINDOW)], axis=0)

    def grads_of(probs, values, upstream, row_dot):
        return (probs * (dot(values, upstream, ((1,), (1,))) - row_dot)).astype(jnp.bfloat16)

    def put_dq(m, h, n, grad_query):
        for g in range(n):
            dq[m, h + g] = grad_query[g * rows:(g + 1) * rows].astype(jnp.bfloat16)

    def hop(c):
        part_of = pl.ds(*plan[c])
        return pltpu.make_async_remote_copy(
            src_ref=dq.at[0, part_of], dst_ref=passed.at[part_of],
            send_sem=hop_send, recv_sem=hop_recv.at[c],
            device_id=below, device_id_type=pl.DeviceIdType.MESH,
        )

    def send_piece(m, o, which, offset, recv_sem):
        pltpu.make_async_remote_copy(
            src_ref=part.at[m, o - 1, which], dst_ref=back.at[m, o - 1, which],
            send_sem=part_send, recv_sem=recv_sem,
            device_id=peer(offset), device_id_type=pl.DeviceIdType.MESH,
        ).start()

    def send_parts(m, dk, dv):
        for o in range(WINDOW - 1, 0, -1):
            for which, total in enumerate((dk, dv)):
                part[m, o - 1, which] = total[(o - 1) * rows:o * rows].astype(jnp.bfloat16)
                send_piece(m, o, which, -o, part_recv.at[m])

    def finish(m):
        if m < micro - 1:
            arrived(back.at[m], part_recv.at[m])
        else:
            @pl.when(first)
            def _():
                arrived(back.at[m], part_recv.at[m])

            @pl.when(jnp.logical_not(first))
            def _():
                arrived(back.at[m, 1], part_recv.at[m])
        for which in range(2):
            total = own[m, which] + back[m, 1, which].astype(jnp.float32)
            beside = back[m, 0, which].astype(jnp.float32)
            if m == micro - 1:
                beside = jnp.where(first, beside, 0.0)
            kv_out[m, which] = (total + beside).astype(jnp.bfloat16)

    log_load.wait()
    arrived(rows_in, rows_sem)
    keys, values = kv[0, 0, 0], kv[0, 0, 1]
    row_dot = []
    for h, n in pairs:
        upstream = split(go[0, :, cols(h, n)])
        row_dot += row_dots(upstream, split(fo[0, :, cols(h, n)]))
        probs = probs_of(0, h, n, keys, own_rows)
        grads = grads_of(probs, values, upstream, joined(row_dot, h, n))
        pr[own_rows, lanes(h, n)] = probs.astype(jnp.bfloat16)
        ds[own_rows, lanes(h, n)] = grads
        dq_own[lanes(h, n), :] = dot(grads, keys, ((0,), (0,)))
        if h == 0:
            send_kv(0, 1, yields)

    take_kv(0, 0)
    keys = far(0, 0)
    for h, n in plan[:1]:
        pf[near_rows, lanes(h, n)] = probs_of(0, h, n, keys, near_rows)
    take_kv(0, 1)
    for m in range(1, micro):
        arrived(kv.at[m, 0], kv_sem.at[m])
        for which in range(2):
            move_kv(m, 0, which, 2, 2)

        @pl.when(first)
        def _(m=m):
            for which in range(2):
                move_kv(m, 0, which, 1, 1)
    values = far(0, 1)
    for c, (h, n) in enumerate(plan):
        upstream = split(go[0, :, cols(h, n)])
        probs = pf[near_rows, lanes(h, n)] if c < 1 else probs_of(0, h, n, keys, near_rows)
        grads = grads_of(probs, values, upstream, joined(row_dot, h, n))
        ds[near_rows, lanes(h, n)] = grads
        put_dq(0, h, n, (dq_own[lanes(h, n), :] + dot(grads, keys, ((0,), (0,)))) * factor)

        @pl.when(has_below if c < early else jnp.logical_and(has_below, first))
        def _(c=c):
            hop(c).start()

        pr[near_rows, lanes(h, n)] = probs.astype(jnp.bfloat16)

    all_queries, all_upstream = split(q[0]), split(go[0])
    dk = dot(ds[...], all_queries, ((1,), (0,))) * factor
    dv = dot(pr[...], all_upstream, ((1,), (0,)))
    send_parts(0, dk[rows:], dv[rows:])
    own[0, 0] = dk[:rows]
    own[0, 1] = dv[:rows]

    for m in range(1, micro):
        for which in range(2):
            take_kv(m, which)
        keys = jnp.concatenate([kv[m, o, 0] for o in range(WINDOW)], axis=0)
        for h, n in pairs:
            pf[:, lanes(h, n)] = probs_of(m, h, n, keys, pl.ds(0, WINDOW * rows))

        far_values, own_values = far(m, 1), kv[m, 0, 1]
        all_queries = split(q[m])
        row_dot = []

        def send_held(who):
            @pl.when(jnp.logical_and(has_below, jnp.logical_and(jnp.logical_not(first), who)))
            def _():
                for held in range(early, len(plan)):
                    hop(held).start()

        def key_sum(h, n):
            return dot(ds[near_rows, lanes(h, n)], all_queries[h * rows:(h + n) * rows], ((1,), (0,)))

        def value_sum(h, n):
            return dot(pr[near_rows, lanes(h, n)], ups[lanes(h, n), :], ((1,), (0,)))

        def send_sum(which, total):
            part[m, 0, which] = total[:rows].astype(jnp.bfloat16)

            @pl.when(first)
            def _():
                send_piece(m, 1, which, 1, relay_recv.at[which])
                part[m, 1, which] = total[rows:].astype(jnp.bfloat16)
                send_piece(m, 2, which, -2, part_recv.at[m])

            @pl.when(jnp.logical_not(first))
            def _():
                send_piece(m, 1, which, -1, part_recv.at[m])
                arrived(back.at[m, 0, which], relay_recv.at[which])
                both = total[rows:] + back[m, 0, which].astype(jnp.float32)
                part[m, 1, which] = both.astype(jnp.bfloat16)
                send_piece(m, 2, which, -2, part_recv.at[m])

        def own_grads(h, n):
            at = lanes(h, n)
            probs = pf[own_rows, at]
            ds[own_rows, at] = grads_of(probs, own_values, ups[at, :], joined(row_dot, h, n))
            pr[own_rows, at] = probs.astype(jnp.bfloat16)

        def sum_far(h, n):
            for which, total in enumerate((key_sum(h, n), value_sum(h, n))):
                far_sum[which] = total if h == 0 else far_sum[which] + total

        for c, (h, n) in enumerate(plan):
            if c == early:
                sum_far(0, h)
                for done, count in pairs[:DONE]:
                    own_grads(done, count)
                if m == 1:
                    send_held(has_above)
            if c == len(plan) - 1:
                sum_far(plan[early][0], h - plan[early][0])
                if m == 1:
                    send_held(jnp.logical_not(has_above))
            if m == 1:
                @pl.when(has_above)
                def _(c=c):
                    hop(c).wait_recv()
            upstream = (
                split(go[m, :, cols(h, n)]).astype(jnp.float32)
                + passed[h:h + n].reshape(n * rows, head).astype(jnp.float32)
            ).astype(jnp.bfloat16)
            ups[lanes(h, n), :] = upstream
            row_dot += row_dots(upstream, split(fo[m, :, cols(h, n)]))
            probs = pf[near_rows, lanes(h, n)]
            pr[near_rows, lanes(h, n)] = probs.astype(jnp.bfloat16)
            grad_probs = dot(far_values, upstream, ((1,), (1,))) - joined(row_dot, h, n)
            if c == len(plan) - 1:
                send_sum(1, far_sum[1] + value_sum(h, n))
            ds[near_rows, lanes(h, n)] = (probs * grad_probs).astype(jnp.bfloat16)
            if c == len(plan) - 1:
                send_sum(0, (far_sum[0] + key_sum(h, n)) * factor)
        for h, n in pairs:
            at = lanes(h, n)
            if h >= DONE * group:
                own_grads(h, n)
            put_dq(m, h, n, dot(ds[:, at], keys, ((0,), (0,))) * factor)
        own[m, 0] = dot(ds[own_rows, :], all_queries, ((1,), (0,))) * factor
        own[m, 1] = dot(pr[own_rows, :], ups[...], ((1,), (0,)))

    for m in range(micro):
        finish(m)
    arrived(kv.at[:, others], kv_send)
    arrived(part, part_send)

    @pl.when(has_below)
    def _():
        arrived(passed, hop_send)


def writer(dq, kv_out, dq_hbm, dk_hbm, dv_hbm, sem):
    micro, heads, _, head = dq.shape
    for m in range(micro):
        for h in range(heads):
            pltpu.make_async_copy(
                dq.at[m, h], dq_hbm.at[0, m, :, pl.ds(h * head, head)], sem.at[0]
            ).start()
        for which, target in enumerate((dk_hbm, dv_hbm)):
            pltpu.make_async_copy(kv_out.at[m, which], target.at[0, m], sem.at[1]).start()
    pltpu.make_async_copy(dq, dq, sem.at[0]).wait()
    pltpu.make_async_copy(kv_out, kv_out, sem.at[1]).wait()


def solution(mesh):
    members = mesh.shape["ctx"]
    sections = mesh.shape["section"]
    in_specs = (
        P("section", None, "ctx", None),
        P("section", None, "ctx", None),
        P("section", None, "ctx", None),
        P("section", None, "ctx", None),
        P("section", None, None, "ctx"),
        P("section", None, "ctx", None),
        P(),
    )
    out_specs = (
        P("section", None, "ctx", None),
        P("section", None, "ctx", None),
        P("section", None, "ctx", None),
    )

    def shards(query_in, key_in, value_in, forward_out, log_sum, grad_out, block_order):
        _, micro, rows, width = query_in.shape
        head = key_in.shape[3]
        heads = width // head
        group = 2 if heads % 2 == 0 else 1
        low, full = jnp.bfloat16, jnp.float32
        dma = pltpu.SemaphoreType.DMA
        others = WINDOW - 1
        dq, kv_out = pl.pallas_call(
            functools.partial(kernel, members, sections, block_order.shape[0]),
            out_shape=(
                pltpu.VMEM((micro, heads, rows, head), low),
                pltpu.VMEM((micro, 2, rows, head), low),
            ),
            in_specs=[pl.BlockSpec(memory_space=pl.ANY)] * 7,
            out_specs=[pl.BlockSpec(memory_space=pltpu.VMEM)] * 2,
            scratch_shapes=[
                pltpu.VMEM((3, micro, rows, width), low),
                pltpu.VMEM((micro, heads, rows), full),
                pltpu.VMEM((micro, WINDOW, 2, rows, head), low),
                pltpu.VMEM((WINDOW * rows, group * rows), full),
                pltpu.VMEM((heads, rows, head), low),
                pltpu.VMEM((micro, 2, rows, head), full),
                pltpu.VMEM((micro, others, 2, rows, head), low),
                pltpu.VMEM((micro, others, 2, rows, head), low),
                pltpu.VMEM((heads * rows, head), full),
                pltpu.VMEM((WINDOW * rows, heads * rows), low),
                pltpu.VMEM((WINDOW * rows, heads * rows), low),
                pltpu.VMEM((WINDOW * rows, heads * rows), full),
                pltpu.VMEM((heads * rows, head), low),
                pltpu.VMEM((2, others * rows, head), full),
                pltpu.SMEM(block_order.shape, jnp.int32),
                dma, dma, dma, dma((micro,)),
                dma, dma((micro,)), dma((micro,)), dma, dma((micro,)), dma((2,)), dma, dma((len(plan_of(heads, group)),)),
            ],
            compiler_params=pltpu.CompilerParams(collective_id=0, has_side_effects=True),
        )(block_order, query_in, key_in, value_in, forward_out, grad_out, log_sum)
        return pl.pallas_call(
            writer,
            out_shape=(
                jax.ShapeDtypeStruct(query_in.shape, low),
                jax.ShapeDtypeStruct(key_in.shape, low),
                jax.ShapeDtypeStruct(value_in.shape, low),
            ),
            in_specs=[pl.BlockSpec(memory_space=pltpu.VMEM)] * 2,
            out_specs=[pl.BlockSpec(memory_space=pl.ANY)] * 3,
            scratch_shapes=[dma((2,))],
        )(*(pltpu.with_memory_space_constraint(x, pltpu.VMEM) for x in (dq, kv_out)))

    return jax.shard_map(shards, mesh=mesh, in_specs=in_specs, out_specs=out_specs, check_vma=False)
```
